8 devices in a mesh: fsdp: 8 (over z, y, x, core).
Axes of the slice: x: 2, y: 2, z: 1, core: 2. Of those that a mesh axis runs over, the one named last changes fastest.
Arguments:
- tokens: int32 [1024, 2], P('fsdp')
- positions: int32 [1024], P('fsdp')
- src_len: int32 [1024], P('fsdp')
- self_k: bfloat16 [2, 1024, 64, 12, 64], P(None, 'fsdp')
- self_v: bfloat16 [2, 1024, 64, 12, 64], P(None, 'fsdp')
- cross_k: bfloat16 [2, 1024, 32, 12, 64], P(None, 'fsdp')
- cross_v: bfloat16 [2, 1024, 32, 12, 64], P(None, 'fsdp')
- attn_w: bfloat16 [2, 6, 768, 768], P(None, None, 'fsdp')
- attn_b: bfloat16 [2, 6, 768], P(None, None, 'fsdp')
- fc1_w: bfloat16 [2, 768, 3072], P(None, 'fsdp')
- fc1_b: bfloat16 [2, 3072], P(None, 'fsdp')
- fc2_w: bfloat16 [2, 3072, 768], P(None, 'fsdp')
- fc2_b: bfloat16 [2, 768], P(None, 'fsdp')
- ln_gain: bfloat16 [2, 3, 768], P(None, None, 'fsdp')
- ln_bias: bfloat16 [2, 3, 768], P(None, None, 'fsdp')
- tok_embed: bfloat16 [50048, 768], P('fsdp')
- pos_embed: bfloat16 [1026, 768], replicated
- emb_norm: bfloat16 [2, 768], replicated
- logit_bias: float32 [50048], P('fsdp')
Outputs:
- output 1: float32 [2, 1024, 50048], P(None, None, 'fsdp')
- output 2: bfloat16 [2, 1024, 64, 12, 64], P(None, 'fsdp')
- output 3: bfloat16 [2, 1024, 64, 12, 64], P(None, 'fsdp')
All inputs are finite; a program needn't handle non-finite values.
Results may differ from the reference program's by a relative error of at most 0.0131539.
Values are sent between devices in bfloat16 or wider.
A program may use at most 1 GiB of HBM per device.

```python
import jax
import jax.numpy as jnp
from jax import lax

D = 768
HEADS = 12
FF = 3072
VOCAB = 50005
VOCAB_PAD = 50048
POS_ROWS = 1026
LAYERS = 2
STEPS = 2
BATCH = 1024
TMAX = 64
SRC = 32

HEAD_DIM = D // HEADS
LN_EPS = 1e-5


def draw_indices(base_key):
    key_tok, key_tpick, key_pos, key_ppick, key_src, key_spick = jax.random.split(base_key, 6)
    flat_ids = jnp.arange(BATCH * STEPS).reshape(BATCH, STEPS)
    tokens = jax.random.randint(key_tok, (BATCH, STEPS), 0, VOCAB)
    tokens = jnp.where(flat_ids == jax.random.randint(key_tpick, (), 0, BATCH * STEPS), VOCAB - 1, tokens)
    row_ids = jnp.arange(BATCH)
    positions = jax.random.randint(key_pos, (BATCH,), 0, TMAX - 1)
    positions = jnp.where(row_ids == jax.random.randint(key_ppick, (), 0, BATCH), TMAX - 2, positions)
    src_len = jax.random.randint(key_src, (BATCH,), 1, SRC + 1)
    src_len = jnp.where(row_ids == jax.random.randint(key_spick, (), 0, BATCH), SRC, src_len)
    return tokens.astype(jnp.int32), positions.astype(jnp.int32), src_len.astype(jnp.int32)


def setup_inputs(seed: int = 0) -> dict:
    key_idx, key_vals = jax.random.split(jax.random.key(seed))
    tokens, positions, src_len = draw_indices(key_idx)
    subkeys = jax.random.split(key_vals, 20)

    def normal(sub_key, out_shape, std_scale):
        return jax.random.normal(sub_key, out_shape, jnp.float32) * std_scale

    cache_shape = (LAYERS, BATCH, TMAX, HEADS, HEAD_DIM)
    cross_shape = (LAYERS, BATCH, SRC, HEADS, HEAD_DIM)
    slot_scale = jnp.array([1.0, 1.0, 1.0, 2.0, 1.0, 2.0], jnp.float32)[None, :, None, None] * D ** -0.5
    vocab_ids = jnp.arange(VOCAB_PAD)
    bias_real = normal(subkeys[17], (VOCAB_PAD,), 0.5)
    bias_pad = jax.random.uniform(subkeys[18], (VOCAB_PAD,), jnp.float32, -12.0, -8.0)
    emb_gain = 1.0 + normal(subkeys[15], (D,), 0.3)
    emb_shift = normal(subkeys[16], (D,), 0.3)
    return {
        'tokens': tokens,
        'positions': positions,
        'src_len': src_len,
        'self_k': normal(subkeys[0], cache_shape, 1.5).astype(jnp.bfloat16),
        'self_v': normal(subkeys[1], cache_shape, 1.0).astype(jnp.bfloat16),
        'cross_k': normal(subkeys[2], cross_shape, 1.5).astype(jnp.bfloat16),
        'cross_v': normal(subkeys[3], cross_shape, 1.0).astype(jnp.bfloat16),
        'attn_w': (normal(subkeys[4], (LAYERS, 6, D, D), 1.0) * slot_scale).astype(jnp.bfloat16),
        'attn_b': normal(subkeys[5], (LAYERS, 6, D), 0.3).astype(jnp.bfloat16),
        'fc1_w': normal(subkeys[6], (LAYERS, D, FF), D ** -0.5).astype(jnp.bfloat16),
        'fc1_b': normal(subkeys[7], (LAYERS, FF), 0.5).astype(jnp.bfloat16),
        'fc2_w': normal(subkeys[8], (LAYERS, FF, D), FF ** -0.5).astype(jnp.bfloat16),
        'fc2_b': normal(subkeys[9], (LAYERS, D), 0.3).astype(jnp.bfloat16),
        'ln_gain': (1.0 + normal(subkeys[10], (LAYERS, 3, D), 0.3)).astype(jnp.bfloat16),
        'ln_bias': normal(subkeys[11], (LAYERS, 3, D), 0.3).astype(jnp.bfloat16),
        'tok_embed': normal(subkeys[12], (VOCAB_PAD, D), D ** -0.5).astype(jnp.bfloat16),
        'pos_embed': normal(subkeys[13], (POS_ROWS, D), D ** -0.5).astype(jnp.bfloat16),
        'emb_norm': jnp.stack([emb_gain, emb_shift]).astype(jnp.bfloat16),
        'logit_bias': jnp.where(vocab_ids < VOCAB, bias_real, bias_pad),
    }


def layer_norm(values, gain_row, shift_row):
    row_mean = values.mean(-1, keepdims=True)
    centered = values - row_mean
    variance = (centered * centered).mean(-1, keepdims=True)
    return centered * lax.rsqrt(variance + LN_EPS) * gain_row.astype(jnp.float32) + shift_row.astype(jnp.float32)


def attend_one(operands):
    query_rows, key_rows, val_rows, valid_len = operands
    scores = jnp.einsum('hd,thd->ht', query_rows.astype(jnp.float32), key_rows.astype(jnp.float32))
    valid_mask = jnp.arange(key_rows.shape[0])[None, :] < valid_len
    scores = jnp.where(valid_mask, scores, -jnp.inf)
    weights = jnp.exp(scores - scores.max(-1, keepdims=True))
    weight_sum = weights.sum(-1, keepdims=True)
    mixed_rows = jnp.einsum('ht,thd->hd', weights.astype(jnp.bfloat16).astype(jnp.float32), val_rows.astype(jnp.float32))
    return mixed_rows / weight_sum


def project(act_rows, weight, bias_row):
    return jnp.dot(act_rows, weight, preferred_element_type=jnp.float32) + bias_row.astype(jnp.float32)


def reference(tokens, positions, src_len, self_k, self_v, cross_k, cross_v, attn_w, attn_b, fc1_w, fc1_b, fc2_w, fc2_b, ln_gain, ln_bias, tok_embed, pos_embed, emb_norm, logit_bias):
    attn_scale = HEAD_DIM ** -0.5
    time_ids = jnp.arange(TMAX)
    cache_k = [self_k[layer_idx] for layer_idx in range(LAYERS)]
    cache_v = [self_v[layer_idx] for layer_idx in range(LAYERS)]
    step_logits = []
    for step_idx in range(STEPS):
        step_pos = positions + step_idx
        start_rows = tok_embed[tokens[:, step_idx]].astype(jnp.float32) + pos_embed[step_pos + 2].astype(jnp.float32)
        hidden = layer_norm(start_rows, emb_norm[0], emb_norm[1])
        write_mask = (time_ids[None, :] == step_pos[:, None])[:, :, None, None]
        for layer_idx in range(LAYERS):
            layer_w = attn_w[layer_idx]
            layer_b = attn_b[layer_idx]
            act_rows = hidden.astype(jnp.bfloat16)
            self_query = (project(act_rows, layer_w[0], layer_b[0]) * attn_scale).astype(jnp.bfloat16).reshape(BATCH, HEADS, HEAD_DIM)
            new_key = project(act_rows, layer_w[1], layer_b[1]).astype(jnp.bfloat16).reshape(BATCH, 1, HEADS, HEAD_DIM)
            new_val = project(act_rows, layer_w[2], layer_b[2]).astype(jnp.bfloat16).reshape(BATCH, 1, HEADS, HEAD_DIM)
            cache_k[layer_idx] = jnp.where(write_mask, new_key, cache_k[layer_idx])
            cache_v[layer_idx] = jnp.where(write_mask, new_val, cache_v[layer_idx])
            mixed_rows = lax.map(attend_one, (self_query, cache_k[layer_idx], cache_v[layer_idx], step_pos + 1))
            attn_out = project(mixed_rows.reshape(BATCH, D).astype(jnp.bfloat16), layer_w[3], layer_b[3])
            hidden = layer_norm(hidden + attn_out, ln_gain[layer_idx, 0], ln_bias[layer_idx, 0])
            cross_query = (project(hidden.astype(jnp.bfloat16), layer_w[4], layer_b[4]) * attn_scale).astype(jnp.bfloat16).reshape(BATCH, HEADS, HEAD_DIM)
            mixed_rows = lax.map(attend_one, (cross_query, cross_k[layer_idx], cross_v[layer_idx], src_len))
            cross_out = project(mixed_rows.reshape(BATCH, D).astype(jnp.bfloat16), layer_w[5], layer_b[5])
            hidden = layer_norm(hidden + cross_out, ln_gain[layer_idx, 1], ln_bias[layer_idx, 1])
            inner_act = jax.nn.gelu(project(hidden.astype(jnp.bfloat16), fc1_w[layer_idx], fc1_b[layer_idx]), approximate=False).astype(jnp.bfloat16)
            ffn_out = project(inner_act, fc2_w[layer_idx], fc2_b[layer_idx])
            hidden = layer_norm(hidden + ffn_out, ln_gain[layer_idx, 2], ln_bias[layer_idx, 2])
        step_logits.append(jnp.dot(hidden.astype(jnp.bfloat16), tok_embed.T, preferred_element_type=jnp.float32) + logit_bias)
    return jnp.stack(step_logits), jnp.stack(cache_k), jnp.stack(cache_v)
```

```python
import functools

import jax
import jax.numpy as jnp
from jax import lax
from jax.experimental import pallas as pl
from jax.experimental.pallas import tpu as pltpu
from jax.sharding import PartitionSpec as P


LN_EPS = 1e-5
F32 = jnp.float32
BF16 = jnp.bfloat16
ERF_SCALE = 0.7071067811865476
SLOTS = 16
NONE = {'transcendentals': 0}
MIB = 2 ** 20


def norm_rows(values, gain, shift):
    mean = jnp.mean(values, axis=-1, keepdims=True)
    centered = values - mean
    var = jnp.mean(centered * centered, axis=-1, keepdims=True)
    return centered * lax.rsqrt(var + LN_EPS) * gain.astype(F32) + shift.astype(F32)


def dot32(a, b):
    return jnp.dot(a, b, preferred_element_type=F32)


MESH = pl.DeviceIdType.MESH
VM = pltpu.VMEM
HBM = pl.BlockSpec(memory_space=pltpu.HBM)


def place():
    me = lax.axis_index('fsdp')
    return (me,) + neighbours(me)


def neighbours(me):
    core, x, y = me % 2, (me // 2) % 2, me // 4
    over_x, over_y = 2 * (1 - 2 * x), 4 * (1 - 2 * y)
    first = me + (1 - core) * over_x + core * over_y
    second = me + (1 - core) * over_y + core * over_x
    return me + 1 - 2 * core, first, second


def owners():
    me, pair, first, second = place()
    far = first + second - me
    _, pair_first, pair_second = neighbours(pair)
    return me, first, second, far, pair, pair_first, pair_second, pair_first + pair_second - pair


PAIR = [(i, i ^ 1) for i in range(8)]
FIRST = [(i, i ^ (4 if i % 2 else 2)) for i in range(8)]
SECOND = [(i, i ^ (2 if i % 2 else 4)) for i in range(8)]


def spread(shard):
    def hop(block, pairs):
        return lax.ppermute(block, 'fsdp', pairs)
    a = hop(shard, FIRST)
    b = hop(shard, SECOND)
    ab = hop(a, SECOND)
    mine = [shard, a, b, ab]
    return mine + [hop(m, PAIR) for m in mine]


def rows_of(owner, part):
    return pl.ds(pl.multiple_of(owner * part, part), part)


def load_slot(shards, slot, dst, sems):
    part = shards[0].shape[1]
    return [pltpu.make_async_copy(ref.at[slot], dst.at[rows_of(own, part)], sems.at[i])
            for i, (ref, own) in enumerate(zip(shards, owners()))]


def begin(copies):
    for c in copies:
        c.start()
    return copies


def finish(copies):
    for c in copies:
        c.wait()


def qkv_kernel(layer, x_ref, wide_ref, *rest):
    shards, (out_ref, w, sems) = rest[:8], rest[8:]
    loads = [begin(load_slot(shards, j, w.at[j], sems.at[j])) for j in range(3)]
    x = x_ref[...].astype(BF16)
    for j in range(3):
        finish(loads[j])
        y = dot32(x, w[j]) + bias_row(wide_ref, layer, j)
        if j == 0:
            y = y * 0.125
        out_ref[j] = y.T.astype(BF16)


def small_kernel(*refs):
    srcs, (wide, ids), outs, (ssem, rsem, lsem) = refs[:6], refs[6:8], refs[8:13], refs[13:]
    dsts = list(outs) + [ids]
    me = lax.axis_index('fsdp')
    barrier = pltpu.get_barrier_semaphore()
    for d in range(1, 8):
        pl.semaphore_signal(barrier, inc=1, device_id=((me + d) % 8,), device_id_type=MESH)
    pl.semaphore_wait(barrier, 7)
    sends, own = [], []
    for i in (5, 0, 1, 2, 3, 4):
        for d in range(1, 8):
            c = pltpu.make_async_remote_copy(src_ref=srcs[i], dst_ref=dsts[i].at[me], send_sem=ssem.at[i, d], recv_sem=rsem.at[i, d],
                                             device_id=((me + d) % 8,), device_id_type=MESH)
            c.start()
            sends.append(c)
        c = pltpu.make_async_copy(srcs[i], dsts[i].at[me], lsem.at[i])
        c.start()
        own.append(c)
    for i in range(6):
        for d in range(1, 8):
            slot = dsts[i].at[(me + 8 - d) % 8]
            pltpu.make_async_remote_copy(src_ref=srcs[i], dst_ref=slot, send_sem=ssem.at[i, d], recv_sem=rsem.at[i, d],
                                         device_id=((me + 8 - d) % 8,), device_id_type=MESH).wait_recv()
    for c in sends:
        c.wait_send()
    finish(own)
    at = 0
    for ref in outs[:3]:
        for j in range(ref.shape[1]):
            wide[at:at + 2] = jnp.concatenate([ref[d, j].astype(F32) for d in range(8)], axis=1)
            at += 2
    wide[at:at + 2] = jnp.concatenate([outs[3][d].astype(F32) for d in range(8)], axis=1)
    at += 2
    for j in range(4):
        wide[at:at + 2] = jnp.concatenate([outs[4][d].astype(F32) for d in (2 * j, 2 * j + 1)], axis=1)
        at += 2


def bias_row(wide_ref, layer, slot):
    return wide_ref[pl.ds(2 * slot + layer, 1), :]


def gain_row(wide_ref, layer, norm):
    return wide_ref[pl.ds(12 + 2 * norm + layer, 1), :], wide_ref[pl.ds(18 + 2 * norm + layer, 1), :]


def greet():
    me, pair, first, second = place()
    barrier = pltpu.get_barrier_semaphore()
    for other in (pair, first, second):
        pl.semaphore_signal(barrier, inc=1, device_id=(other,), device_id_type=MESH)
    pl.semaphore_wait(barrier, 3)
    return me, pair, first, second


def embed_kernel(vocab, src, ids, pos_rows, norm_ref, out, r1, s1, r2, s2, r3, ssem, rsem):
    me, pair, first, second = greet()
    core = me % 2

    def send(k, block, dst, device):
        c = pltpu.make_async_remote_copy(src_ref=block, dst_ref=dst, send_sem=ssem.at[k], recv_sem=rsem.at[k],
                                         device_id=(device,), device_id_type=MESH)
        c.start()
        return c
    def chips(at):
        c, cx, cy = at % 2, (at // 2) % 2, at // 4
        flip_x, flip_y = 1 - 2 * cx, 2 * (1 - 2 * cy)
        here = at // 2
        f = here + (1 - c) * flip_x + c * flip_y
        g = here + (1 - c) * flip_y + c * flip_x
        return here, g, f, f + g - here
    def held(block, dest, owner):
        parts = []
        for s in range(ids.shape[1]):
            row = ids[dest, pl.ds(s, 1), :] - owner * vocab
            here = jnp.where((row >= 0) & (row < vocab), 1.0, 0.0)
            tile = jnp.broadcast_to(here, (128, 128)).T.astype(BF16)
            parts.append(block[s * 128:(s + 1) * 128] * jnp.concatenate([tile] * (block.shape[1] // 128), axis=1))
        return jnp.concatenate(parts, axis=0)
    mine = chips(me)
    theirs = chips(pair)
    step = [send(j, src.at[theirs[j] * 2 + (1 - core)], r1.at[j], pair) for j in (2, 3, 1, 0)]
    order = (2, 3, 1, 0)
    hops = {}
    for n, j in enumerate(order):
        step[n].wait()
        dest = mine[j] * 2 + core
        s1[j] = held(src[dest], dest, me) + held(r1[j], dest, pair)
        if j >= 2:
            hops[j] = send(4 + j, s1.at[j], r2.at[j - 2], first)
    for j in (3, 2):
        hops[j].wait()
    s2[...] = s1[1] + r2[1]
    last = send(8, s2, r3, second)
    s1[0] = s1[0] + r2[0]
    last.wait()
    start = (s1[0] + r3[...]).astype(F32) + pos_rows[...].astype(F32)
    out[...] = norm_rows(start, norm_ref[0:1], norm_ref[1:2])


def gather_kernel(src, out, ssem, rsem, lsem):
    me, pair, first, second = greet()
    far = first + second - me
    _, pair_first, pair_second = neighbours(pair)
    pair_far = pair_first + pair_second - pair
    local = pltpu.make_async_copy(src, out.at[me], lsem)
    local.start()

    def send(k, s, block, slot, device):
        c = pltpu.make_async_remote_copy(src_ref=block, dst_ref=out.at[slot, s], send_sem=ssem.at[k, s], recv_sem=rsem.at[k, s],
                                         device_id=(device,), device_id_type=MESH)
        c.start()
        return c

    def arrive(k, s, slot, device):
        pltpu.make_async_remote_copy(src_ref=out.at[slot, s], dst_ref=out.at[slot, s], send_sem=ssem.at[k, s], recv_sem=rsem.at[k, s],
                                     device_id=(device,), device_id_type=MESH).wait_recv()
    sent = []
    halves = range(src.shape[0])
    for s in halves:
        sent.append(send(0, s, src.at[s], me, first))
        sent.append(send(1, s, src.at[s], me, second))
        sent.append(send(3, s, src.at[s], me, pair))
    for s in halves:
        arrive(0, s, first, first)
        sent.append(send(2, s, out.at[first, s], first, second))
        sent.append(send(4, s, out.at[first, s], first, pair))
        arrive(1, s, second, second)
        sent.append(send(5, s, out.at[second, s], second, pair))
    for s in halves:
        arrive(2, s, far, second)
        sent.append(send(6, s, out.at[far, s], far, pair))
    for s in halves:
        arrive(3, s, pair, pair)
        arrive(4, s, pair_first, pair)
        arrive(5, s, pair_second, pair)
        arrive(6, s, pair_far, pair)
    for c in sent:
        c.wait_send()
    local.wait()


GROUP = 8


def scores_of(k_ref, q0, q1, s0_ref, s1_ref, times, write=None):
    def trip(i, carry):
        base = pl.multiple_of(i * GROUP, GROUP)
        rows0, rows1 = [], []
        for j in range(GROUP):
            raw = k_ref[base + j]
            kt = raw.astype(F32)
            rows0.append(jnp.sum(kt * q0, axis=0, keepdims=True))
            rows1.append(jnp.sum(kt * q1, axis=0, keepdims=True))
            if write is not None:
                write(base + j, raw)
        s0_ref[pl.ds(base, GROUP), :] = jnp.concatenate(rows0, axis=0)
        s1_ref[pl.ds(base, GROUP), :] = jnp.concatenate(rows1, axis=0)
        return carry
    lax.fori_loop(0, times // GROUP, trip, 0)


def mix_of(v_ref, w0_ref, w1_ref, times, init, write=None):
    def trip(i, carry):
        o0, o1 = carry
        base = pl.multiple_of(i * GROUP, GROUP)
        for j in range(GROUP):
            raw = v_ref[base + j]
            vt = raw.astype(F32)
            o0 = o0 + vt * w0_ref[pl.ds(base + j, 1), :]
            o1 = o1 + vt * w1_ref[pl.ds(base + j, 1), :]
            if write is not None:
                write(base + j, raw)
        return o0, o1
    return lax.fori_loop(0, times // GROUP, trip, init)


def soften(scores, mask):
    scores = jnp.where(mask, scores, -jnp.inf)
    weights = jnp.exp(scores - jnp.max(scores, axis=0, keepdims=True))
    return weights, jnp.sum(weights, axis=0, keepdims=True)


def self_kernel(*refs):
    for head in range(refs[1].shape[1]):
        self_head(head, *refs)


def self_head(head, pos_ref, q_ref, kn_ref, vn_ref, k_ref, v_ref, *rest):
    o_ref, ko_ref, vo_ref, s0_ref, s1_ref = rest[-5:]
    times, dim, lanes = k_ref.shape[1], k_ref.shape[3], k_ref.shape[4]
    kc, vc = k_ref.at[0, :, head], v_ref.at[0, :, head]
    pos = pos_ref[...]
    q = q_ref[0, head].astype(F32)
    kn = kn_ref[0, head]
    vn = vn_ref[0, head]
    q0, q1 = q[:, :lanes], q[:, lanes:]
    k0, k1 = kn[:, :lanes], kn[:, lanes:]
    v0, v1 = vn[:, :lanes], vn[:, lanes:]
    pack = 16
    here_b = jnp.broadcast_to(pos.astype(F32), (pack, lanes)).astype(BF16)
    after_b = jnp.broadcast_to((pos + 1).astype(F32), (pack, lanes)).astype(BF16)

    def writer(out_ref, new0, new1):
        def write(time, raw):
            step = jnp.broadcast_to(lax.convert_element_type(time, F32), (pack, lanes)).astype(BF16)
            first, second = here_b == step, after_b == step
            for r in range(0, dim, pack):
                rows = slice(r, r + pack)
                out_ref[0, time, head, rows] = jnp.where(first, new0[rows], jnp.where(second, new1[rows], raw[rows]))
        return write
    scores_of(kc, q0, q1, s0_ref, s1_ref, times, writer(ko_ref, k0, k1))
    s00 = jnp.sum(q0 * k0.astype(F32), axis=0, keepdims=True)
    s10 = jnp.sum(q1 * k0.astype(F32), axis=0, keepdims=True)
    s11 = jnp.sum(q1 * k1.astype(F32), axis=0, keepdims=True)
    t = lax.broadcasted_iota(jnp.int32, (times, lanes), 0)
    here, after = t == pos, t == pos + 1
    w0, sum0 = soften(jnp.where(here, s00, s0_ref[...]), t <= pos)
    w1, sum1 = soften(jnp.where(here, s10, jnp.where(after, s11, s1_ref[...])), t <= pos + 1)
    w0 = w0.astype(BF16).astype(F32)
    w1 = w1.astype(BF16).astype(F32)
    w00 = jnp.sum(jnp.where(here, w0, 0.0), axis=0, keepdims=True)
    w10 = jnp.sum(jnp.where(here, w1, 0.0), axis=0, keepdims=True)
    w11 = jnp.sum(jnp.where(after, w1, 0.0), axis=0, keepdims=True)
    s0_ref[...] = jnp.where(here, 0.0, w0)
    s1_ref[...] = jnp.where(here | after, 0.0, w1)
    o0, o1 = mix_of(vc, s0_ref, s1_ref, times,
                    (w00 * v0.astype(F32), w10 * v0.astype(F32) + w11 * v1.astype(F32)), writer(vo_ref, v0, v1))
    o_ref[head, :, :lanes] = (o0 / sum0).astype(BF16)
    o_ref[head, :, lanes:] = (o1 / sum1).astype(BF16)


def cross_kernel(*refs):
    for head in range(refs[1].shape[0]):
        cross_head(head, *refs)


def cross_head(head, len_ref, q_ref, k_ref, v_ref, o_ref, s0_ref, s1_ref):
    times, lanes = k_ref.shape[1], k_ref.shape[4]
    q = q_ref[head].astype(F32)
    scores_of(k_ref.at[0, :, head], q[:, :lanes], q[:, lanes:], s0_ref, s1_ref, times)
    mask = lax.broadcasted_iota(jnp.int32, (times, lanes), 0) < len_ref[...]
    w0, sum0 = soften(s0_ref[...], mask)
    w1, sum1 = soften(s1_ref[...], mask)
    s0_ref[...] = w0.astype(BF16).astype(F32)
    s1_ref[...] = w1.astype(BF16).astype(F32)
    zero = jnp.zeros((k_ref.shape[3], lanes), F32)
    o0, o1 = mix_of(v_ref.at[0, :, head], s0_ref, s1_ref, times, (zero, zero))
    o_ref[head, :, :lanes] = (o0 / sum0).astype(BF16)
    o_ref[head, :, lanes:] = (o1 / sum1).astype(BF16)


def turn(o_ref):
    return o_ref[...].astype(F32).T.astype(BF16)


def mid_kernel(layer, h_ref, o_ref, wide_ref, *rest):
    shards, (h_out, q_out, w, sems) = rest[:8], rest[8:]
    loads = [begin(load_slot(shards, 3 + j, w.at[j], sems.at[j])) for j in range(2)]
    o = turn(o_ref)
    finish(loads[0])
    h = h_ref[...] + (dot32(o, w[0]) + bias_row(wide_ref, layer, 3))
    h = norm_rows(h, *gain_row(wide_ref, layer, 0))
    h_out[...] = h
    finish(loads[1])
    q = (dot32(h.astype(BF16), w[1]) + bias_row(wide_ref, layer, 4)) * 0.125
    q_out[...] = q.T.astype(BF16)


def ffn_kernel(layer, h_ref, o_ref, wide_ref, *rest):
    shards, inner_shards, (h_out, hb_out, w, up, down, sems) = rest[:8], rest[8:16], rest[16:]
    part = shards[0].shape[1]
    width = h_ref.shape[1]
    blocks = up.shape[0]
    first = begin(load_slot(shards, 5, w, sems.at[0]))
    ups = [begin(load_slot(inner_shards, j, up.at[j], sems.at[1 + j])) for j in range(blocks)]
    downs = begin([pltpu.make_async_copy(ref.at[pl.ds(blocks, blocks)], down.at[own], sems.at[1 + blocks, i])
                   for i, (ref, own) in enumerate(zip(inner_shards, owners()))])
    o = turn(o_ref)
    finish(first)
    h = h_ref[...] + (dot32(o, w[...]) + bias_row(wide_ref, layer, 5))
    h = norm_rows(h, *gain_row(wide_ref, layer, 1))
    act = h.astype(BF16)
    acc = h + bias_row(wide_ref, layer, 12)
    per = width // (blocks * part)
    for j in range(blocks):
        finish(ups[j])
        u = dot32(act, up[j]) + bias_row(wide_ref, layer, 13 + j)
        g = (0.5 * u * (1.0 + lax.erf(u * ERF_SCALE))).astype(BF16)
        if j == 0:
            finish(downs)
        acc = acc + dot32(g, down[j * per:(j + 1) * per].reshape(width, width))
    h = norm_rows(acc, *gain_row(wide_ref, layer, 2))
    h_out[...] = h
    for i in range(hb_out.shape[0]):
        lanes = hb_out.shape[2]
        hb_out[i] = h[i * lanes:(i + 1) * lanes].T.astype(BF16)


def logits_kernel(hid_ref, tok_ref, bias_ref, out_ref, joined, bias):
    shards, _, _, lanes = hid_ref.shape
    tile = tok_ref.shape[0]
    step = pl.program_id(1)

    @pl.when(pl.program_id(0) == 0)
    def _():
        for i in range(shards):
            joined[step, :, i * lanes:(i + 1) * lanes] = hid_ref[i, step]

    @pl.when(step == 0)
    def _():
        for i in range(0, bias.shape[0], lanes):
            bias[i:i + lanes] = jnp.broadcast_to(bias_ref[0, :, i:i + lanes], (lanes, lanes)).T
    y = dot32(tok_ref[...], joined[step])
    for i in range(shards):
        cols = slice(i * lanes, (i + 1) * lanes)
        out_ref[0, :, cols] = y[:, cols] + bias[:tile]


def pack_kernel(up_ref, down_ref, out_ref):
    blocks, part, width = out_ref.shape[0] // 2, out_ref.shape[1], out_ref.shape[2]
    for j in range(blocks):
        out_ref[j] = up_ref[0, :, j * width:(j + 1) * width]
        out_ref[blocks + j] = down_ref[0, j * part:(j + 1) * part]


def params(limit_mib, sem='arbitrary'):
    return pltpu.CompilerParams(vmem_limit_bytes=limit_mib * MIB, dimension_semantics=(sem,))


def whole(shape):
    return pl.BlockSpec(shape, lambda i: (0,) * len(shape))


def run_small(*srcs):
    width = 8 * srcs[0].shape[-1]
    shapes = [(SLOTS,) + x.shape for x in srcs]
    return pl.pallas_call(
        small_kernel, name='small_gather',
        out_shape=(jax.ShapeDtypeStruct((40, width), F32), jax.ShapeDtypeStruct(shapes[5], jnp.int32)),
        in_specs=[pl.BlockSpec(memory_space=VM)] * 6, out_specs=[pl.BlockSpec(memory_space=VM)] * 2,
        scratch_shapes=[VM(shape, BF16) for shape in shapes[:5]] + [pltpu.SemaphoreType.DMA((6, 8)), pltpu.SemaphoreType.DMA((6, 8)), pltpu.SemaphoreType.DMA((6,))],
        compiler_params=pltpu.CompilerParams(collective_id=0, has_side_effects=True, vmem_limit_bytes=16 * MIB),
        cost_estimate=pl.CostEstimate(flops=4000000, bytes_accessed=1000000, **NONE),
    )(*srcs)


def run_embed(picked, ids, pos_rows, norm, vocab):
    _, rows, width = picked.shape
    block = VM((rows, width), BF16)
    return pl.pallas_call(
        functools.partial(embed_kernel, vocab), name='embed_sum',
        out_shape=jax.ShapeDtypeStruct((rows, width), F32),
        in_specs=[pl.BlockSpec(memory_space=VM)] * 4, out_specs=pl.BlockSpec(memory_space=VM),
        scratch_shapes=[VM((4, rows, width), BF16), VM((4, rows, width), BF16), VM((2, rows, width), BF16), block, block,
                        pltpu.SemaphoreType.DMA((9,)), pltpu.SemaphoreType.DMA((9,))],
        compiler_params=pltpu.CompilerParams(collective_id=1, has_side_effects=True, vmem_limit_bytes=32 * MIB),
        cost_estimate=pl.CostEstimate(flops=20000000, bytes_accessed=picked.size * 4, **NONE),
    )(picked, ids, pos_rows, norm)


def run_gather(rows):
    return pl.pallas_call(
        gather_kernel, name='row_gather',
        out_shape=jax.ShapeDtypeStruct((8,) + rows.shape, rows.dtype),
        in_specs=[pl.BlockSpec(memory_space=VM)], out_specs=pl.BlockSpec(memory_space=VM),
        scratch_shapes=[pltpu.SemaphoreType.DMA((7, rows.shape[0])), pltpu.SemaphoreType.DMA((7, rows.shape[0])), pltpu.SemaphoreType.DMA],
        compiler_params=pltpu.CompilerParams(collective_id=2, has_side_effects=True, vmem_limit_bytes=32 * MIB),
        cost_estimate=pl.CostEstimate(flops=20000000, bytes_accessed=rows.size * 18, **NONE),
    )(rows)


def run_qkv(layer, x, shards, wide):
    rows, width = x.shape
    return pl.pallas_call(
        functools.partial(qkv_kernel, layer), grid=(1,), name='qkv',
        out_shape=jax.ShapeDtypeStruct((3, width, rows), BF16),
        in_specs=[whole((rows, width)), whole(wide.shape)] + [HBM] * 8,
        out_specs=whole((3, width, rows)),
        scratch_shapes=[VM((3, width, width), BF16), pltpu.SemaphoreType.DMA((3, 8))],
        compiler_params=params(53),
        cost_estimate=pl.CostEstimate(flops=2 * rows * width * width * 3, bytes_accessed=6 * width * width, **NONE),
    )(x, wide, *shards)


def run_self(layer, pos, qkv, cache_k, cache_v, new_k, new_v, per=2):
    _, times, heads, dim, lanes = cache_k.shape
    rows = qkv.shape[-1]
    qkv = qkv.reshape(3, heads, dim, rows)
    cache_spec = pl.BlockSpec((1, times, per, dim, lanes), lambda h: (layer, 0, h, 0, 0))
    args = [pos, qkv, qkv, qkv, cache_k, cache_v]
    specs = [whole((1, lanes))] + [pl.BlockSpec((1, per, dim, rows), functools.partial(lambda j, h: (j, h, 0, 0), j)) for j in range(3)]
    specs += [cache_spec, cache_spec]
    aliases = {}
    if new_k is not None:
        args += [new_k, new_v]
        specs += [pl.BlockSpec(memory_space=pl.ANY)] * 2
        aliases = {6: 1, 7: 2}
    return pl.pallas_call(
        self_kernel, grid=(heads // per,), name='self_attn',
        out_shape=(jax.ShapeDtypeStruct((heads, dim, rows), BF16),
                   jax.ShapeDtypeStruct(cache_k.shape, BF16), jax.ShapeDtypeStruct(cache_v.shape, BF16)),
        in_specs=specs,
        out_specs=(pl.BlockSpec((per, dim, rows), lambda h: (h, 0, 0)), cache_spec, cache_spec),
        scratch_shapes=[VM((times, lanes), F32), VM((times, lanes), F32)],
        input_output_aliases=aliases,
        compiler_params=params(53),
        cost_estimate=pl.CostEstimate(flops=8 * heads * dim * rows * times, bytes_accessed=8 * times * heads * dim * lanes, **NONE),
    )(*args)


def run_cross(layer, lens, q, cross_k, cross_v, per=3):
    _, times, heads, dim, lanes = cross_k.shape
    rows = q.shape[-1]
    q = q.reshape(heads, dim, rows)
    spec = pl.BlockSpec((1, times, per, dim, lanes), lambda h: (layer, 0, h, 0, 0))
    row_spec = pl.BlockSpec((per, dim, rows), lambda h: (h, 0, 0))
    return pl.pallas_call(
        cross_kernel, grid=(heads // per,), name='cross_attn',
        out_shape=jax.ShapeDtypeStruct((heads, dim, rows), BF16),
        in_specs=[whole((1, lanes)), row_spec, spec, spec],
        out_specs=row_spec,
        scratch_shapes=[VM((times, lanes), F32), VM((times, lanes), F32)],
        compiler_params=params(53),
        cost_estimate=pl.CostEstimate(flops=8 * heads * dim * rows * times, bytes_accessed=4 * times * heads * dim * lanes, **NONE),
    )(lens, q, cross_k, cross_v)


def run_mid(layer, h, o, shards, wide):
    rows, width = h.shape
    return pl.pallas_call(
        functools.partial(mid_kernel, layer), grid=(1,), name='mid',
        out_shape=(jax.ShapeDtypeStruct((rows, width), F32), jax.ShapeDtypeStruct((width, rows), BF16)),
        in_specs=[whole((rows, width)), whole((width, rows)), whole(wide.shape)] + [HBM] * 8,
        out_specs=(whole((rows, width)), whole((width, rows))),
        scratch_shapes=[VM((2, width, width), BF16), pltpu.SemaphoreType.DMA((2, 8))],
        compiler_params=params(53),
        cost_estimate=pl.CostEstimate(flops=4 * rows * width * width, bytes_accessed=4 * width * width, **NONE),
    )(h, o.reshape(width, rows), wide, *shards)


def run_ffn(layer, h, o, shards, inner_shards, wide):
    rows, width = h.shape
    part = shards[0].shape[1]
    blocks = inner_shards[0].shape[0] // 2
    inner = blocks * width
    return pl.pallas_call(
        functools.partial(ffn_kernel, layer), grid=(1,), name='ffn',
        out_shape=(jax.ShapeDtypeStruct((rows, width), F32), jax.ShapeDtypeStruct((2, width, rows // 2), BF16)),
        in_specs=[whole((rows, width)), whole((width, rows)), whole(wide.shape)] + [HBM] * 16,
        out_specs=(whole((rows, width)), whole((2, width, rows // 2))),
        scratch_shapes=[VM((width, width), BF16), VM((blocks, width, width), BF16), VM((8, blocks, part, width), BF16),
                        pltpu.SemaphoreType.DMA((blocks + 2, 8))],
        compiler_params=params(53),
        cost_estimate=pl.CostEstimate(flops=4 * rows * width * inner, bytes_accessed=4 * width * inner, **NONE),
    )(h, o.reshape(width, rows), wide, *shards, *inner_shards)


def run_pack(layer, up, down):
    _, part, inner = up.shape
    width = down.shape[2]
    return pl.pallas_call(
        pack_kernel, grid=(1,), name='pack',
        out_shape=jax.ShapeDtypeStruct((2 * inner // width, part, width), BF16),
        in_specs=[pl.BlockSpec((1, part, inner), lambda i: (layer, 0, 0)), pl.BlockSpec((1,) + down.shape[1:], lambda i: (layer, 0, 0))],
        out_specs=whole((2 * inner // width, part, width)),
        compiler_params=params(16),
        cost_estimate=pl.CostEstimate(flops=2000000, bytes_accessed=8 * part * inner, **NONE),
    )(up, down)


def run_logits(hid, tok, bias, tile=1568):
    shards, steps, width, lanes = hid.shape
    vocab = tok.shape[0]
    rows = shards * lanes
    tiles = pl.cdiv(vocab, tile)
    bias = jnp.pad(bias, (0, tiles * tile - vocab)).reshape(tiles, 1, tile)
    bias = jnp.pad(bias, ((0, 0), (0, 0), (0, -tile % lanes)))
    return pl.pallas_call(
        logits_kernel, grid=(tiles, steps), name='logits',
        out_shape=jax.ShapeDtypeStruct((steps, vocab, rows), F32),
        in_specs=[pl.BlockSpec(hid.shape, lambda v, s: (0, 0, 0, 0)),
                  pl.BlockSpec((tile, width), lambda v, s: (v, 0)),
                  pl.BlockSpec((1, 1, bias.shape[2]), lambda v, s: (v, 0, 0))],
        out_specs=pl.BlockSpec((1, tile, rows), lambda v, s: (s, v, 0)),
        scratch_shapes=[VM((steps, width, rows), BF16), VM((bias.shape[2], lanes), F32)],
        compiler_params=pltpu.CompilerParams(vmem_limit_bytes=56 * MIB, dimension_semantics=('arbitrary', 'arbitrary')),
        cost_estimate=pl.CostEstimate(flops=2 * steps * rows * vocab * width, bytes_accessed=4 * steps * rows * vocab, **NONE),
    )(hid, tok, bias)


def solution(mesh):
    cache_spec = P(None, 'fsdp')
    in_specs = (P('fsdp'), P('fsdp'), P('fsdp'), cache_spec, cache_spec, cache_spec, cache_spec,
                P(None, None, 'fsdp'), P(None, None, 'fsdp'), P(None, 'fsdp'), P(None, 'fsdp'),
                P(None, 'fsdp'), P(None, 'fsdp'), P(None, None, 'fsdp'), P(None, None, 'fsdp'),
                P('fsdp'), P(), P(), P('fsdp'))
    out_specs = (P(None, None, 'fsdp'), cache_spec, cache_spec)


    def decode(tokens, positions, src_len, self_k, self_v, cross_k, cross_v, attn_w, attn_b, fc1_w, fc1_b, fc2_w, fc2_b, ln_gain, ln_bias, tok_embed, pos_embed, emb_norm, logit_bias):
        me = lax.axis_index('fsdp')
        shards = lax.axis_size('fsdp')
        layers = attn_w.shape[0]
        _, steps = tokens.shape
        width = attn_w.shape[3]
        vocab = tok_embed.shape[0]

        flip = lambda z: z.transpose(1, 0, 2)
        wide, ids = run_small(flip(attn_b), flip(ln_gain), flip(ln_bias), fc2_b, fc1_b, tokens.T)
        local_ids = jnp.clip(ids[:shards].reshape(-1) - me * vocab, 0, vocab - 1)
        picked = tok_embed.at[local_ids].get(mode='promise_in_bounds').reshape(shards, -1, width)
        row_pos = jnp.concatenate([positions + 2 + s for s in range(steps)])
        pos_rows = pos_embed.at[row_pos].get(mode='promise_in_bounds')
        hidden = run_embed(picked, ids, pos_rows, emb_norm, vocab)

        to_lanes = (0, 2, 3, 4, 1)
        old_k, old_v, ck, cv = [c.transpose(to_lanes) for c in (self_k, self_v, cross_k, cross_v)]
        pos = positions[None, :]
        lens = src_len[None, :]
        new_k = new_v = None
        after = [wide, hidden]
        attn = [attn_w[layer] for layer in range(layers)]
        inner = [run_pack(layer, fc1_w, fc2_w) for layer in range(layers)]
        attn[0], _ = lax.optimization_barrier((attn[0], after[0]))
        inner[0], _ = lax.optimization_barrier((inner[0], after[1]))
        attn_shards = [spread(attn[layer]) for layer in range(layers)]
        inner_shards = [spread(inner[layer]) for layer in range(layers)]
        for layer in range(layers):
            w = attn_shards[layer]
            qkv = run_qkv(layer, hidden, w, wide)
            o, new_k, new_v = run_self(layer, pos, qkv, old_k, old_v, new_k, new_v)
            hidden, q = run_mid(layer, hidden, o, w, wide)
            o = run_cross(layer, lens, q, ck, cv)
            hidden, hidden_b = run_ffn(layer, hidden, o, w, inner_shards[layer], wide)
        rows = run_gather(hidden_b)
        logits = run_logits(rows, tok_embed, logit_bias)
        back = (0, 4, 1, 2, 3)
        return logits.transpose(0, 2, 1), new_k.transpose(back), new_v.transpose(back)

    return jax.shard_map(decode, mesh=mesh, in_specs=in_specs, out_specs=out_specs, check_vma=False)
```

```python
import functools

import jax
import jax.numpy as jnp
from jax import lax
from jax.experimental import pallas as pl
from jax.experimental.pallas import tpu as pltpu
from jax.sharding import PartitionSpec as P


LN_EPS = 1e-5
F32 = jnp.float32
BF16 = jnp.bfloat16
ERF_SCALE = 0.7071067811865476
SLOTS = 16
MIB = 2 ** 20


def norm_rows(values, gain, shift):
    mean = jnp.mean(values, axis=-1, keepdims=True)
    centered = values - mean
    var = jnp.mean(centered * centered, axis=-1, keepdims=True)
    return centered * lax.rsqrt(var + LN_EPS) * gain.astype(F32) + shift.astype(F32)


def dot32(a, b):
    return jnp.dot(a, b, preferred_element_type=F32)


MESH = pl.DeviceIdType.MESH
VM = pltpu.VMEM
HBM = pl.BlockSpec(memory_space=pltpu.HBM)


def place():
    me = lax.axis_index('fsdp')
    return (me,) + neighbours(me)


def neighbours(me):
    core, x, y = me % 2, (me // 2) % 2, me // 4
    over_x, over_y = 2 * (1 - 2 * x), 4 * (1 - 2 * y)
    first = me + (1 - core) * over_x + core * over_y
    second = me + (1 - core) * over_y + core * over_x
    return me + 1 - 2 * core, first, second


def owners():
    me, pair, first, second = place()
    far = first + second - me
    _, pair_first, pair_second = neighbours(pair)
    return me, first, second, far, pair, pair_first, pair_second, pair_first + pair_second - pair


PAIR = [(i, i ^ 1) for i in range(8)]
FIRST = [(i, i ^ (4 if i % 2 else 2)) for i in range(8)]
SECOND = [(i, i ^ (2 if i % 2 else 4)) for i in range(8)]


def spread(shard):
    def hop(block, pairs):
        return lax.ppermute(block, 'fsdp', pairs)

    a = hop(shard, FIRST)
    b = hop(shard, SECOND)
    ab = hop(a, SECOND)
    mine = [shard, a, b, ab]
    return mine + [hop(m, PAIR) for m in mine]


def rows_of(owner, part):
    return pl.ds(pl.multiple_of(owner * part, part), part)


def load_slot(shards, slot, dst, sems):
    part = shards[0].shape[1]
    return [pltpu.make_async_copy(ref.at[slot], dst.at[rows_of(own, part)], sems.at[i])
            for i, (ref, own) in enumerate(zip(shards, owners()))]


def begin(copies):
    for c in copies:
        c.start()
    return copies


def finish(copies):
    for c in copies:
        c.wait()


def qkv_kernel(layer, x_ref, wide_ref, *rest):
    shards, (out_ref, w, sems) = rest[:8], rest[8:]
    loads = [begin(load_slot(shards, j, w.at[j], sems.at[j])) for j in range(3)]
    x = x_ref[...].astype(BF16)
    for j in range(3):
        finish(loads[j])
        y = dot32(x, w[j]) + bias_row(wide_ref, layer, j)
        if j == 0:
            y = y * 0.125
        out_ref[j] = y.T.astype(BF16)


def small_kernel(*refs):
    srcs, (wide, ids), outs, (ssem, rsem, lsem) = refs[:6], refs[6:8], refs[8:13], refs[13:]
    dsts = list(outs) + [ids]
    me = lax.axis_index('fsdp')
    barrier = pltpu.get_barrier_semaphore()
    for d in range(1, 8):
        pl.semaphore_signal(barrier, inc=1, device_id=((me + d) % 8,), device_id_type=MESH)
    pl.semaphore_wait(barrier, 7)
    sends, own = [], []
    for i in (5, 0, 1, 2, 3, 4):
        for d in range(1, 8):
            c = pltpu.make_async_remote_copy(src_ref=srcs[i], dst_ref=dsts[i].at[me], send_sem=ssem.at[i, d], recv_sem=rsem.at[i, d],
                                             device_id=((me + d) % 8,), device_id_type=MESH)
            c.start()
            sends.append(c)
        c = pltpu.make_async_copy(srcs[i], dsts[i].at[me], lsem.at[i])
        c.start()
        own.append(c)
    for i in range(6):
        for d in range(1, 8):
            slot = dsts[i].at[(me + 8 - d) % 8]
            pltpu.make_async_remote_copy(src_ref=srcs[i], dst_ref=slot, send_sem=ssem.at[i, d], recv_sem=rsem.at[i, d],
                                         device_id=((me + 8 - d) % 8,), device_id_type=MESH).wait_recv()
    for c in sends:
        c.wait_send()
    finish(own)
    at = 0
    for ref in outs[:3]:
        for j in range(ref.shape[1]):
            wide[at:at + 2] = jnp.concatenate([ref[d, j].astype(F32) for d in range(8)], axis=1)
            at += 2
    wide[at:at + 2] = jnp.concatenate([outs[3][d].astype(F32) for d in range(8)], axis=1)
    at += 2
    for j in range(4):
        wide[at:at + 2] = jnp.concatenate([outs[4][d].astype(F32) for d in (2 * j, 2 * j + 1)], axis=1)
        at += 2


def bias_row(wide_ref, layer, slot):
    return wide_ref[pl.ds(2 * slot + layer, 1), :]


def gain_row(wide_ref, layer, norm):
    return wide_ref[pl.ds(12 + 2 * norm + layer, 1), :], wide_ref[pl.ds(18 + 2 * norm + layer, 1), :]


def greet():
    me, pair, first, second = place()
    barrier = pltpu.get_barrier_semaphore()
    for other in (pair, first, second):
        pl.semaphore_signal(barrier, inc=1, device_id=(other,), device_id_type=MESH)
    pl.semaphore_wait(barrier, 3)
    return me, pair, first, second


def embed_kernel(vocab, src, ids, pos_rows, norm_ref, out, r1, s1, r2, s2, r3, ssem, rsem):
    me, pair, first, second = greet()
    core = me % 2

    def send(k, block, dst, device):
        c = pltpu.make_async_remote_copy(src_ref=block, dst_ref=dst, send_sem=ssem.at[k], recv_sem=rsem.at[k],
                                         device_id=(device,), device_id_type=MESH)
        c.start()
        return c

    def chips(at):
        c, cx, cy = at % 2, (at // 2) % 2, at // 4
        flip_x, flip_y = 1 - 2 * cx, 2 * (1 - 2 * cy)
        here = at // 2
        f = here + (1 - c) * flip_x + c * flip_y
        g = here + (1 - c) * flip_y + c * flip_x
        return here, g, f, f + g - here

    def held(block, dest, owner):
        parts = []
        for s in range(ids.shape[1]):
            row = ids[dest, pl.ds(s, 1), :] - owner * vocab
            here = jnp.where((row >= 0) & (row < vocab), 1.0, 0.0)
            tile = jnp.broadcast_to(here, (128, 128)).T.astype(BF16)
            parts.append(block[s * 128:(s + 1) * 128] * jnp.concatenate([tile] * (block.shape[1] // 128), axis=1))
        return jnp.concatenate(parts, axis=0)

    mine = chips(me)
    theirs = chips(pair)
    step = [send(j, src.at[theirs[j] * 2 + (1 - core)], r1.at[j], pair) for j in (2, 3, 1, 0)]
    order = (2, 3, 1, 0)
    hops = {}
    for n, j in enumerate(order):
        step[n].wait()
        dest = mine[j] * 2 + core
        s1[j] = held(src[dest], dest, me) + held(r1[j], dest, pair)
        if j >= 2:
            hops[j] = send(4 + j, s1.at[j], r2.at[j - 2], first)
    for j in (3, 2):
        hops[j].wait()
    s2[...] = s1[1] + r2[1]
    last = send(8, s2, r3, second)
    s1[0] = s1[0] + r2[0]
    last.wait()
    start = (s1[0] + r3[...]).astype(F32) + pos_rows[...].astype(F32)
    out[...] = norm_rows(start, norm_ref[0:1], norm_ref[1:2])


def gather_kernel(src, out, ssem, rsem, lsem):
    me, pair, first, second = greet()
    far = first + second - me
    _, pair_first, pair_second = neighbours(pair)
    pair_far = pair_first + pair_second - pair
    local = pltpu.make_async_copy(src, out.at[me], lsem)
    local.start()

    def send(k, s, block, slot, device):
        c = pltpu.make_async_remote_copy(src_ref=block, dst_ref=out.at[slot, s], send_sem=ssem.at[k, s], recv_sem=rsem.at[k, s],
                                         device_id=(device,), device_id_type=MESH)
        c.start()
        return c

    def arrive(k, s, slot, device):
        pltpu.make_async_remote_copy(src_ref=out.at[slot, s], dst_ref=out.at[slot, s], send_sem=ssem.at[k, s], recv_sem=rsem.at[k, s],
                                     device_id=(device,), device_id_type=MESH).wait_recv()

    sent = []
    halves = range(src.shape[0])
    for s in halves:
        sent.append(send(0, s, src.at[s], me, first))
        sent.append(send(1, s, src.at[s], me, second))
        sent.append(send(3, s, src.at[s], me, pair))
    for s in halves:
        arrive(0, s, first, first)
        sent.append(send(2, s, out.at[first, s], first, second))
        sent.append(send(4, s, out.at[first, s], first, pair))
        arrive(1, s, second, second)
        sent.append(send(5, s, out.at[second, s], second, pair))
    for s in halves:
        arrive(2, s, far, second)
        sent.append(send(6, s, out.at[far, s], far, pair))
    for s in halves:
        arrive(3, s, pair, pair)
        arrive(4, s, pair_first, pair)
        arrive(5, s, pair_second, pair)
        arrive(6, s, pair_far, pair)
    for c in sent:
        c.wait_send()
    local.wait()


GROUP = 8


def scores_of(k_ref, q0, q1, s0_ref, s1_ref, times, write=None):
    def trip(i, carry):
        base = pl.multiple_of(i * GROUP, GROUP)
        rows0, rows1 = [], []
        for j in range(GROUP):
            raw = k_ref[base + j]
            kt = raw.astype(F32)
            rows0.append(jnp.sum(kt * q0, axis=0, keepdims=True))
            rows1.append(jnp.sum(kt * q1, axis=0, keepdims=True))
            if write is not None:
                write(base + j, raw)
        s0_ref[pl.ds(base, GROUP), :] = jnp.concatenate(rows0, axis=0)
        s1_ref[pl.ds(base, GROUP), :] = jnp.concatenate(rows1, axis=0)
        return carry

    lax.fori_loop(0, times // GROUP, trip, 0)


def mix_of(v_ref, w0_ref, w1_ref, times, init, write=None):
    def trip(i, carry):
        o0, o1 = carry
        base = pl.multiple_of(i * GROUP, GROUP)
        for j in range(GROUP):
            raw = v_ref[base + j]
            vt = raw.astype(F32)
            o0 = o0 + vt * w0_ref[pl.ds(base + j, 1), :]
            o1 = o1 + vt * w1_ref[pl.ds(base + j, 1), :]
            if write is not None:
                write(base + j, raw)
        return o0, o1

    return lax.fori_loop(0, times // GROUP, trip, init)


def soften(scores, mask):
    scores = jnp.where(mask, scores, -jnp.inf)
    weights = jnp.exp(scores - jnp.max(scores, axis=0, keepdims=True))
    return weights, jnp.sum(weights, axis=0, keepdims=True)


def self_kernel(layer, *refs):
    heads_in, (h_ref, wide_ref), shards = refs[:6], refs[6:8], refs[8:16]
    h_out, q_out, ko_ref, vo_ref, o, w, sems, s0_ref, s1_ref = refs[-9:]
    step = pl.program_id(0)
    per = heads_in[1].shape[1]

    def loads(j):
        return load_slot(shards, 3 + j, w.at[j], sems.at[j])

    @pl.when(step == 0)
    def _():
        begin(loads(0) + loads(1))

    for head in range(per):
        self_head(head, *heads_in, o.at[pl.ds(step * per, per)], ko_ref, vo_ref, s0_ref, s1_ref)

    @pl.when(step == pl.num_programs(0) - 1)
    def _():
        finish(loads(0) + loads(1))
        h = h_ref[...] + (dot32(turn(o), w[0]) + bias_row(wide_ref, layer, 3))
        h = norm_rows(h, *gain_row(wide_ref, layer, 0))
        h_out[...] = h
        q = (dot32(h.astype(BF16), w[1]) + bias_row(wide_ref, layer, 4)) * 0.125
        q_out[...] = q.T.astype(BF16)


def self_head(head, pos_ref, q_ref, kn_ref, vn_ref, k_ref, v_ref, *rest):
    o_ref, ko_ref, vo_ref, s0_ref, s1_ref = rest[-5:]
    times, dim, lanes = k_ref.shape[1], k_ref.shape[3], k_ref.shape[4]
    kc, vc = k_ref.at[0, :, head], v_ref.at[0, :, head]
    pos = pos_ref[...]
    q = q_ref[0, head].astype(F32)
    kn = kn_ref[0, head]
    vn = vn_ref[0, head]
    q0, q1 = q[:, :lanes], q[:, lanes:]
    k0, k1 = kn[:, :lanes], kn[:, lanes:]
    v0, v1 = vn[:, :lanes], vn[:, lanes:]
    pack = 16
    here_b = jnp.broadcast_to(pos.astype(F32), (pack, lanes)).astype(BF16)
    after_b = jnp.broadcast_to((pos + 1).astype(F32), (pack, lanes)).astype(BF16)

    def writer(out_ref, new0, new1):
        def write(time, raw):
            step = jnp.broadcast_to(lax.convert_element_type(time, F32), (pack, lanes)).astype(BF16)
            first, second = here_b == step, after_b == step
            for r in range(0, dim, pack):
                rows = slice(r, r + pack)
                out_ref[0, time, head, rows] = jnp.where(first, new0[rows], jnp.where(second, new1[rows], raw[rows]))

        return write

    scores_of(kc, q0, q1, s0_ref, s1_ref, times, writer(ko_ref, k0, k1))
    s00 = jnp.sum(q0 * k0.astype(F32), axis=0, keepdims=True)
    s10 = jnp.sum(q1 * k0.astype(F32), axis=0, keepdims=True)
    s11 = jnp.sum(q1 * k1.astype(F32), axis=0, keepdims=True)
    t = lax.broadcasted_iota(jnp.int32, (times, lanes), 0)
    here, after = t == pos, t == pos + 1
    w0, sum0 = soften(jnp.where(here, s00, s0_ref[...]), t <= pos)
    w1, sum1 = soften(jnp.where(here, s10, jnp.where(after, s11, s1_ref[...])), t <= pos + 1)
    w0 = w0.astype(BF16).astype(F32)
    w1 = w1.astype(BF16).astype(F32)
    w00 = jnp.sum(jnp.where(here, w0, 0.0), axis=0, keepdims=True)
    w10 = jnp.sum(jnp.where(here, w1, 0.0), axis=0, keepdims=True)
    w11 = jnp.sum(jnp.where(after, w1, 0.0), axis=0, keepdims=True)
    s0_ref[...] = jnp.where(here, 0.0, w0)
    s1_ref[...] = jnp.where(here | after, 0.0, w1)
    o0, o1 = mix_of(vc, s0_ref, s1_ref, times,
                    (w00 * v0.astype(F32), w10 * v0.astype(F32) + w11 * v1.astype(F32)), writer(vo_ref, v0, v1))
    o_ref[head, :, :lanes] = (o0 / sum0).astype(BF16)
    o_ref[head, :, lanes:] = (o1 / sum1).astype(BF16)


def cross_kernel(layer, *refs):
    heads_in, (h_ref, wide_ref), shards = refs[:4], refs[4:6], refs[6:14]
    h_out, o, w, sems, s0_ref, s1_ref = refs[14:]
    step = pl.program_id(0)
    per = heads_in[1].shape[0]

    def loads():
        return load_slot(shards, 5, w, sems)

    @pl.when(step == 0)
    def _():
        begin(loads())

    for head in range(per):
        cross_head(head, *heads_in, o.at[pl.ds(step * per, per)], s0_ref, s1_ref)

    @pl.when(step == pl.num_programs(0) - 1)
    def _():
        finish(loads())
        h = h_ref[...] + (dot32(turn(o), w[...]) + bias_row(wide_ref, layer, 5))
        h_out[...] = norm_rows(h, *gain_row(wide_ref, layer, 1))


def cross_head(head, len_ref, q_ref, k_ref, v_ref, o_ref, s0_ref, s1_ref):
    times, lanes = k_ref.shape[1], k_ref.shape[4]
    q = q_ref[head].astype(F32)
    scores_of(k_ref.at[0, :, head], q[:, :lanes], q[:, lanes:], s0_ref, s1_ref, times)
    mask = lax.broadcasted_iota(jnp.int32, (times, lanes), 0) < len_ref[...]
    w0, sum0 = soften(s0_ref[...], mask)
    w1, sum1 = soften(s1_ref[...], mask)
    s0_ref[...] = w0.astype(BF16).astype(F32)
    s1_ref[...] = w1.astype(BF16).astype(F32)
    zero = jnp.zeros((k_ref.shape[3], lanes), F32)
    o0, o1 = mix_of(v_ref.at[0, :, head], s0_ref, s1_ref, times, (zero, zero))
    o_ref[head, :, :lanes] = (o0 / sum0).astype(BF16)
    o_ref[head, :, lanes:] = (o1 / sum1).astype(BF16)


def turn(o_ref):
    heads, dim, rows = o_ref.shape
    return o_ref[...].reshape(heads * dim, rows).astype(F32).T.astype(BF16)


def ffn_kernel(layer, h_ref, wide_ref, *rest):
    inner_shards, (h_out, hb_out, up, down, sems) = rest[:8], rest[8:]
    part = inner_shards[0].shape[1]
    width = h_ref.shape[1]
    blocks = up.shape[0]
    ups = [begin(load_slot(inner_shards, j, up.at[j], sems.at[j])) for j in range(blocks)]
    downs = begin([pltpu.make_async_copy(ref.at[pl.ds(blocks, blocks)], down.at[own], sems.at[blocks, i])
                   for i, (ref, own) in enumerate(zip(inner_shards, owners()))])
    h = h_ref[...]
    act = h.astype(BF16)
    acc = h + bias_row(wide_ref, layer, 12)
    per = width // (blocks * part)
    for j in range(blocks):
        finish(ups[j])
        u = dot32(act, up[j]) + bias_row(wide_ref, layer, 13 + j)
        g = (0.5 * u * (1.0 + lax.erf(u * ERF_SCALE))).astype(BF16)
        if j == 0:
            finish(downs)
        acc = acc + dot32(g, down[j * per:(j + 1) * per].reshape(width, width))
    h = norm_rows(acc, *gain_row(wide_ref, layer, 2))
    h_out[...] = h
    for i in range(hb_out.shape[0]):
        lanes = hb_out.shape[2]
        hb_out[i] = h[i * lanes:(i + 1) * lanes].T.astype(BF16)


def logits_kernel(hid_ref, tok_ref, bias_ref, out_ref, joined, bias):
    shards, _, _, lanes = hid_ref.shape
    tile = tok_ref.shape[0]
    step = pl.program_id(1)

    @pl.when(pl.program_id(0) == 0)
    def _():
        for i in range(shards):
            joined[step, :, i * lanes:(i + 1) * lanes] = hid_ref[i, step]

    @pl.when(step == 0)
    def _():
        for i in range(0, bias.shape[0], lanes):
            bias[i:i + lanes] = jnp.broadcast_to(bias_ref[0, :, i:i + lanes], (lanes, lanes)).T

    y = dot32(tok_ref[...], joined[step])
    for i in range(shards):
        cols = slice(i * lanes, (i + 1) * lanes)
        out_ref[0, :, cols] = y[:, cols] + bias[:tile]


def pack_kernel(up_ref, down_ref, out_ref):
    blocks, part, width = out_ref.shape[0] // 2, out_ref.shape[1], out_ref.shape[2]
    for j in range(blocks):
        out_ref[j] = up_ref[0, :, j * width:(j + 1) * width]
        out_ref[blocks + j] = down_ref[0, j * part:(j + 1) * part]


def params(limit_mib, sem='arbitrary'):
    return pltpu.CompilerParams(vmem_limit_bytes=limit_mib * MIB, dimension_semantics=(sem,))


def cost(flops):
    return pl.CostEstimate(flops=flops, bytes_accessed=flops, transcendentals=0)


def whole(shape):
    return pl.BlockSpec(shape, lambda i: (0,) * len(shape))


def run_small(*srcs):
    width = 8 * srcs[0].shape[-1]
    shapes = [(SLOTS,) + x.shape for x in srcs]
    return pl.pallas_call(
        small_kernel, name='small_gather',
        out_shape=(jax.ShapeDtypeStruct((40, width), F32), jax.ShapeDtypeStruct(shapes[5], jnp.int32)),
        in_specs=[pl.BlockSpec(memory_space=VM)] * 6, out_specs=[pl.BlockSpec(memory_space=VM)] * 2,
        scratch_shapes=[VM(shape, BF16) for shape in shapes[:5]] + [pltpu.SemaphoreType.DMA((6, 8)), pltpu.SemaphoreType.DMA((6, 8)), pltpu.SemaphoreType.DMA((6,))],
        compiler_params=pltpu.CompilerParams(collective_id=0, has_side_effects=True, vmem_limit_bytes=16 * MIB),
        cost_estimate=cost(4000000),
    )(*srcs)


def run_embed(picked, ids, pos_rows, norm, vocab):
    _, rows, width = picked.shape
    block = VM((rows, width), BF16)
    return pl.pallas_call(
        functools.partial(embed_kernel, vocab), name='embed_sum',
        out_shape=jax.ShapeDtypeStruct((rows, width), F32),
        in_specs=[pl.BlockSpec(memory_space=VM)] * 4, out_specs=pl.BlockSpec(memory_space=VM),
        scratch_shapes=[VM((4, rows, width), BF16), VM((4, rows, width), BF16), VM((2, rows, width), BF16), block, block,
                        pltpu.SemaphoreType.DMA((9,)), pltpu.SemaphoreType.DMA((9,))],
        compiler_params=pltpu.CompilerParams(collective_id=1, has_side_effects=True, vmem_limit_bytes=32 * MIB),
        cost_estimate=cost(20000000),
    )(picked, ids, pos_rows, norm)


def run_gather(rows):
    return pl.pallas_call(
        gather_kernel, name='row_gather',
        out_shape=jax.ShapeDtypeStruct((8,) + rows.shape, rows.dtype),
        in_specs=[pl.BlockSpec(memory_space=VM)], out_specs=pl.BlockSpec(memory_space=VM),
        scratch_shapes=[pltpu.SemaphoreType.DMA((7, rows.shape[0])), pltpu.SemaphoreType.DMA((7, rows.shape[0])), pltpu.SemaphoreType.DMA],
        compiler_params=pltpu.CompilerParams(collective_id=2, has_side_effects=True, vmem_limit_bytes=32 * MIB),
        cost_estimate=cost(20000000),
    )(rows)


def run_qkv(layer, x, shards, wide):
    rows, width = x.shape
    return pl.pallas_call(
        functools.partial(qkv_kernel, layer), grid=(1,), name='qkv',
        out_shape=jax.ShapeDtypeStruct((3, width, rows), BF16),
        in_specs=[whole((rows, width)), whole(wide.shape)] + [HBM] * 8,
        out_specs=whole((3, width, rows)),
        scratch_shapes=[VM((3, width, width), BF16), pltpu.SemaphoreType.DMA((3, 8))],
        compiler_params=params(53),
        cost_estimate=cost(2 * rows * width * width * 3),
    )(x, wide, *shards)


def run_self(layer, pos, qkv, cache_k, cache_v, new, h, shards, wide, per=2):
    _, times, heads, dim, lanes = cache_k.shape
    rows, width = h.shape
    qkv = qkv.reshape(3, heads, dim, rows)
    cache_spec = pl.BlockSpec((1, times, per, dim, lanes), lambda i: (layer, 0, i, 0, 0))
    args = [pos, qkv, qkv, qkv, cache_k, cache_v, h, wide, *shards]
    specs = [whole((1, lanes))] + [pl.BlockSpec((1, per, dim, rows), functools.partial(lambda j, i: (j, i, 0, 0), j)) for j in range(3)]
    specs += [cache_spec, cache_spec, whole(h.shape), whole(wide.shape)] + [HBM] * len(shards)
    aliases = {len(args) + i: 2 + i for i in range(len(new))}
    return pl.pallas_call(
        functools.partial(self_kernel, layer), grid=(heads // per,), name='self_attn',
        out_shape=(jax.ShapeDtypeStruct(h.shape, F32), jax.ShapeDtypeStruct((width, rows), BF16),
                   jax.ShapeDtypeStruct(cache_k.shape, BF16), jax.ShapeDtypeStruct(cache_v.shape, BF16)),
        in_specs=specs + [HBM] * len(new),
        out_specs=(whole(h.shape), whole((width, rows)), cache_spec, cache_spec),
        scratch_shapes=[VM((heads, dim, rows), BF16), VM((2, width, width), BF16), pltpu.SemaphoreType.DMA((2, 8)),
                        VM((times, lanes), F32), VM((times, lanes), F32)],
        input_output_aliases=aliases,
        compiler_params=params(53), cost_estimate=cost(8 * heads * dim * rows * times),
    )(*args, *new)


def run_cross(layer, lens, q, cross_k, cross_v, h, shards, wide, per=3):
    _, times, heads, dim, lanes = cross_k.shape
    rows, width = h.shape
    q = q.reshape(heads, dim, rows)
    spec = pl.BlockSpec((1, times, per, dim, lanes), lambda i: (layer, 0, i, 0, 0))
    return pl.pallas_call(
        functools.partial(cross_kernel, layer), grid=(heads // per,), name='cross_attn',
        out_shape=jax.ShapeDtypeStruct(h.shape, F32),
        in_specs=[whole((1, lanes)), pl.BlockSpec((per, dim, rows), lambda i: (i, 0, 0)), spec, spec, whole(h.shape), whole(wide.shape)] + [HBM] * len(shards),
        out_specs=whole(h.shape),
        scratch_shapes=[VM((heads, dim, rows), BF16), VM((width, width), BF16), pltpu.SemaphoreType.DMA((8,)),
                        VM((times, lanes), F32), VM((times, lanes), F32)],
        compiler_params=params(53), cost_estimate=cost(8 * heads * dim * rows * times),
    )(lens, q, cross_k, cross_v, h, wide, *shards)


def run_ffn(layer, h, inner_shards, wide):
    rows, width = h.shape
    part = inner_shards[0].shape[1]
    blocks = inner_shards[0].shape[0] // 2
    inner = blocks * width
    return pl.pallas_call(
        functools.partial(ffn_kernel, layer), grid=(1,), name='ffn',
        out_shape=(jax.ShapeDtypeStruct((rows, width), F32), jax.ShapeDtypeStruct((2, width, rows // 2), BF16)),
        in_specs=[whole((rows, width)), whole(wide.shape)] + [HBM] * 8,
        out_specs=(whole((rows, width)), whole((2, width, rows // 2))),
        scratch_shapes=[VM((blocks, width, width), BF16), VM((8, blocks, part, width), BF16),
                        pltpu.SemaphoreType.DMA((blocks + 1, 8))],
        compiler_params=params(53),
        cost_estimate=cost(4 * rows * width * inner),
    )(h, wide, *inner_shards)


def run_pack(layer, up, down):
    _, part, inner = up.shape
    width = down.shape[2]
    return pl.pallas_call(
        pack_kernel, grid=(1,), name='pack',
        out_shape=jax.ShapeDtypeStruct((2 * inner // width, part, width), BF16),
        in_specs=[pl.BlockSpec((1, part, inner), lambda i: (layer, 0, 0)), pl.BlockSpec((1,) + down.shape[1:], lambda i: (layer, 0, 0))],
        out_specs=whole((2 * inner // width, part, width)),
        compiler_params=params(16),
        cost_estimate=cost(2000000),
    )(up, down)


def run_logits(hid, tok, bias, tile=1568):
    shards, steps, width, lanes = hid.shape
    vocab = tok.shape[0]
    rows = shards * lanes
    tiles = pl.cdiv(vocab, tile)
    bias = jnp.pad(bias, (0, tiles * tile - vocab)).reshape(tiles, 1, tile)
    bias = jnp.pad(bias, ((0, 0), (0, 0), (0, -tile % lanes)))
    return pl.pallas_call(
        logits_kernel, grid=(tiles, steps), name='logits',
        out_shape=jax.ShapeDtypeStruct((steps, vocab, rows), F32),
        in_specs=[pl.BlockSpec(hid.shape, lambda v, s: (0, 0, 0, 0)),
                  pl.BlockSpec((tile, width), lambda v, s: (v, 0)),
                  pl.BlockSpec((1, 1, bias.shape[2]), lambda v, s: (v, 0, 0))],
        out_specs=pl.BlockSpec((1, tile, rows), lambda v, s: (s, v, 0)),
        scratch_shapes=[VM((steps, width, rows), BF16), VM((bias.shape[2], lanes), F32)],
        compiler_params=pltpu.CompilerParams(vmem_limit_bytes=56 * MIB, dimension_semantics=('arbitrary', 'arbitrary')),
        cost_estimate=cost(2 * steps * rows * vocab * width),
    )(hid, tok, bias)


def solution(mesh):
    cache_spec = P(None, 'fsdp')
    in_specs = (P('fsdp'), P('fsdp'), P('fsdp'), cache_spec, cache_spec, cache_spec, cache_spec,
                P(None, None, 'fsdp'), P(None, None, 'fsdp'), P(None, 'fsdp'), P(None, 'fsdp'),
                P(None, 'fsdp'), P(None, 'fsdp'), P(None, None, 'fsdp'), P(None, None, 'fsdp'),
                P('fsdp'), P(), P(), P('fsdp'))
    out_specs = (P(None, None, 'fsdp'), cache_spec, cache_spec)


    def decode(tokens, positions, src_len, self_k, self_v, cross_k, cross_v, attn_w, attn_b, fc1_w, fc1_b, fc2_w, fc2_b, ln_gain, ln_bias, tok_embed, pos_embed, emb_norm, logit_bias):
        me = lax.axis_index('fsdp')
        shards = lax.axis_size('fsdp')
        layers = attn_w.shape[0]
        _, steps = tokens.shape
        width = attn_w.shape[3]
        vocab = tok_embed.shape[0]

        flip = lambda z: z.transpose(1, 0, 2)
        wide, ids = run_small(flip(attn_b), flip(ln_gain), flip(ln_bias), fc2_b, fc1_b, tokens.T)
        local_ids = jnp.clip(ids[:shards].reshape(-1) - me * vocab, 0, vocab - 1)
        picked = tok_embed.at[local_ids].get(mode='promise_in_bounds').reshape(shards, -1, width)
        row_pos = jnp.concatenate([positions + 2 + s for s in range(steps)])
        pos_rows = pos_embed.at[row_pos].get(mode='promise_in_bounds')
        hidden = run_embed(picked, ids, pos_rows, emb_norm, vocab)

        to_lanes = (0, 2, 3, 4, 1)
        old_k, old_v, ck, cv = [c.transpose(to_lanes) for c in (self_k, self_v, cross_k, cross_v)]
        pos = positions[None, :]
        lens = src_len[None, :]
        new = ()
        after = [wide, hidden]
        later, _ = lax.optimization_barrier((attn_w, picked))
        attn = [attn_w[0]] + [later[layer] for layer in range(1, layers)]
        inner = [run_pack(layer, fc1_w, fc2_w) for layer in range(layers)]
        attn[0], _ = lax.optimization_barrier((attn[0], after[0]))
        inner[0], _ = lax.optimization_barrier((inner[0], after[1]))
        attn_shards = [spread(attn[layer]) for layer in range(layers)]
        inner_shards = [spread(inner[layer]) for layer in range(layers)]
        for layer in range(layers):
            w = attn_shards[layer]
            qkv = run_qkv(layer, hidden, w, wide)
            hidden, q, *new = run_self(layer, pos, qkv, old_k, old_v, new, hidden, w, wide)
            hidden = run_cross(layer, lens, q, ck, cv, hidden, w, wide)
            hidden, hidden_b = run_ffn(layer, hidden, inner_shards[layer], wide)
        rows = run_gather(hidden_b)
        logits = run_logits(rows, tok_embed, logit_bias)
        back = (0, 4, 1, 2, 3)
        return logits.transpose(0, 2, 1), *[z.transpose(back) for z in new]

    return jax.shard_map(decode, mesh=mesh, in_specs=in_specs, out_specs=out_specs, check_vma=False)
```
